32 devices in a mesh: pod: 1 (over z), data: 4 (over y), expert: 8 (over x, core).
Axes of the slice: x: 4, y: 4, z: 1, core: 2. Of those that a mesh axis runs over, the one named last changes fastest.
The devices are a block of a 4x4x8 slice.
Arguments:
- tokens: bfloat16 [16384, 1536], P(('pod', 'data', 'expert'))
- routes: int32 [16384, 8], P(('pod', 'data', 'expert'))
- gates: float32 [16384, 8], P(('pod', 'data', 'expert'))
- grad_y: bfloat16 [16384, 1536], P(('pod', 'data', 'expert'))
- w_in1: bfloat16 [40, 1536, 512], P('expert')
- w_in3: bfloat16 [40, 1536, 512], P('expert')
- w_out: bfloat16 [40, 512, 1536], P('expert')
Outputs:
- output 1: bfloat16 [16384, 1536], P(('pod', 'data', 'expert'))
- output 2: bfloat16 [16384, 1536], P(('pod', 'data', 'expert'))
- output 3: float32 [40, 1536, 512], P(('pod', 'expert'))
- output 4: float32 [40, 1536, 512], P(('pod', 'expert'))
- output 5: float32 [40, 512, 1536], P(('pod', 'expert'))
All inputs are finite; a program needn't handle non-finite values.
Results may differ from the reference program's by a relative error of at most 0.0051087.
Values are sent between devices in bfloat16 or wider.
A program may use at most 768 MiB of HBM per device.

```python
import functools
import jax
import jax.numpy as jnp
from jax import lax

D_MODEL = 1536
D_FF = 512
N_EXPERTS = 40
TOP_K = 8
TOK_DEV = 512
N_DATA = 4
N_EXPERT_DEV = 8
CAP_COLD = 104
CAP_HOT = 192
N_HOT = 2

GROUPS = N_DATA * N_EXPERT_DEV
TOK_PART = GROUPS * TOK_DEV


def hot_index_table(expert_ids):
    return jnp.where(expert_ids == 0, 0, jnp.where(expert_ids == N_EXPERTS // 2, 1, -1))


def draw_routes(key):
    key_hot, key_pos, key_base_a, key_base_b, key_step = jax.random.split(key, 5)
    n_cold = N_EXPERTS - N_HOT
    pattern = jnp.concatenate([
        jnp.zeros((CAP_HOT,), jnp.int32),
        jnp.ones((CAP_HOT,), jnp.int32),
        jnp.full((TOK_DEV - N_HOT * CAP_HOT,), -1, jnp.int32)])
    hot_of_tok = jax.random.permutation(key_hot, pattern)
    hot_slot = jax.random.randint(key_pos, (TOK_DEV, 1), 0, TOP_K)
    base_rank = jnp.minimum(jax.random.randint(key_base_a, (TOK_DEV, 1), 0, n_cold),
                            jax.random.randint(key_base_b, (TOK_DEV, 1), 0, n_cold))
    step_max = max(1, (n_cold - 1) // max(TOP_K - 1, 1))
    step_size = jax.random.randint(key_step, (TOK_DEV, 1), 1, step_max + 1)
    slot_ids = jnp.arange(TOP_K)[None, :]
    cold_rank = (base_rank + slot_ids * step_size) % n_cold
    cold_expert = cold_rank + 1 + (cold_rank + 1 >= N_EXPERTS // 2).astype(jnp.int32)
    use_hot = (hot_of_tok[:, None] >= 0) & (slot_ids == hot_slot)
    return jnp.where(use_hot, hot_of_tok[:, None] * (N_EXPERTS // 2), cold_expert).astype(jnp.int32)


def setup_inputs(seed: int = 0, part: int = 0) -> dict:
    key = jax.random.key(seed)
    key_part = jax.random.fold_in(key, part)
    key_tok, key_route, key_gate, key_grad = jax.random.split(key_part, 4)
    key_one, key_three, key_two = jax.random.split(jax.random.fold_in(key, 99991), 3)
    routes = jax.vmap(draw_routes)(jax.random.split(key_route, GROUPS)).reshape(TOK_PART, TOP_K)
    tokens = jax.random.normal(key_tok, (TOK_PART, D_MODEL), jnp.float32).astype(jnp.bfloat16)
    gates = jax.random.uniform(key_gate, (TOK_PART, TOP_K), jnp.float32, 0.5, 1.5)
    grad_y = jax.random.normal(key_grad, (TOK_PART, D_MODEL), jnp.float32).astype(jnp.bfloat16)
    w_in1 = (jax.random.normal(key_one, (N_EXPERTS, D_MODEL, D_FF), jnp.float32) * D_MODEL ** -0.5).astype(jnp.bfloat16)
    w_in3 = (jax.random.normal(key_three, (N_EXPERTS, D_MODEL, D_FF), jnp.float32) * D_MODEL ** -0.5).astype(jnp.bfloat16)
    w_out = (jax.random.normal(key_two, (N_EXPERTS, D_FF, D_MODEL), jnp.float32) * D_FF ** -0.5).astype(jnp.bfloat16)
    return dict(tokens=tokens, routes=routes, gates=gates, grad_y=grad_y, w_in1=w_in1, w_in3=w_in3, w_out=w_out)


def route_rows(routes_dev):
    flat_exp = routes_dev.reshape(-1)
    n_slots = flat_exp.shape[0]
    order = jnp.argsort(flat_exp, stable=True)
    counts = jax.ops.segment_sum(jnp.ones((n_slots,), jnp.int32), flat_exp, num_segments=N_EXPERTS)
    starts = jnp.cumsum(counts) - counts
    rank_sorted = jnp.arange(n_slots, dtype=jnp.int32) - starts[flat_exp[order]]
    slot_rank = jnp.zeros((n_slots,), jnp.int32).at[order].set(rank_sorted)
    hot_index = hot_index_table(flat_exp)
    cold_row = jnp.where((hot_index < 0) & (slot_rank < CAP_COLD), flat_exp * CAP_COLD + slot_rank, N_EXPERTS * CAP_COLD)
    hot_row = jnp.where(hot_index >= 0, hot_index * CAP_HOT + slot_rank, N_HOT * CAP_HOT)
    return cold_row, hot_row


def gather_rows(slot_rows, x_local, dy_local, gate_flat, n_rows):
    n_slots = slot_rows.shape[0]
    tok_n = x_local.shape[0]
    top_k = n_slots // tok_n
    src_tok = jnp.full((n_rows,), tok_n, jnp.int32).at[slot_rows].set(
        jnp.arange(n_slots, dtype=jnp.int32) // top_k, mode='drop')
    src_gate = jnp.zeros((n_rows,), jnp.float32).at[slot_rows].set(gate_flat, mode='drop')
    x_rows = jnp.take(x_local, src_tok, axis=0, mode='fill', fill_value=0)
    dy_rows = jnp.take(dy_local, src_tok, axis=0, mode='fill', fill_value=0)
    do_rows = (dy_rows.astype(jnp.float32) * src_gate[:, None]).astype(jnp.bfloat16)
    return x_rows, do_rows


def expert_pass(x_rows, do_rows, w_a, w_b, w_c):
    pre_a = jnp.dot(x_rows, w_a, preferred_element_type=jnp.float32).astype(jnp.bfloat16)
    pre_b = jnp.dot(x_rows, w_b, preferred_element_type=jnp.float32).astype(jnp.bfloat16)
    act_a = pre_a.astype(jnp.float32)
    act_b = pre_b.astype(jnp.float32)
    sigma_a = jax.nn.sigmoid(act_a)
    hidden = (act_a * sigma_a * act_b).astype(jnp.bfloat16)
    outs = jnp.dot(hidden, w_c, preferred_element_type=jnp.float32).astype(jnp.bfloat16)
    d_hidden = jnp.dot(do_rows, w_c.T, preferred_element_type=jnp.float32)
    d_pre_b = (d_hidden * act_a * sigma_a).astype(jnp.bfloat16)
    d_pre_a = (d_hidden * act_b * sigma_a * (1.0 + act_a * (1.0 - sigma_a))).astype(jnp.bfloat16)
    d_rows = (jnp.dot(d_pre_a, w_a.T, preferred_element_type=jnp.float32)
              + jnp.dot(d_pre_b, w_b.T, preferred_element_type=jnp.float32)).astype(jnp.bfloat16)
    grad_a = jnp.dot(x_rows.T, d_pre_a, preferred_element_type=jnp.float32)
    grad_b = jnp.dot(x_rows.T, d_pre_b, preferred_element_type=jnp.float32)
    grad_c = jnp.dot(hidden.T, do_rows, preferred_element_type=jnp.float32)
    return outs, d_rows, grad_a, grad_b, grad_c


def run_expert(operands):
    return expert_pass(*operands)


def combine(cold_rows, hot_rows, cold_vals, hot_vals, weights):
    slot_vals = (jnp.take(cold_vals, cold_rows, axis=0, mode='fill', fill_value=0)
                 + jnp.take(hot_vals, hot_rows, axis=0, mode='fill', fill_value=0))
    weighted = weights.reshape(TOK_DEV, TOP_K, 1) * slot_vals.reshape(TOK_DEV, TOP_K, D_MODEL).astype(jnp.float32)
    return jnp.sum(weighted, axis=1).astype(jnp.bfloat16)


def by_expert(buffers, n_buf, cap):
    return buffers.reshape(GROUPS, n_buf, cap, D_MODEL).transpose(1, 0, 2, 3).reshape(n_buf, GROUPS * cap, D_MODEL)


def by_device(buffers, n_buf, cap):
    return buffers.reshape(n_buf, GROUPS, cap, D_MODEL).transpose(1, 0, 2, 3).reshape(GROUPS, n_buf * cap, D_MODEL)


def reference(tokens, routes, gates, grad_y, w_in1, w_in3, w_out):
    x_dev = tokens.reshape(GROUPS, TOK_DEV, D_MODEL)
    dy_dev = grad_y.reshape(GROUPS, TOK_DEV, D_MODEL)
    gate_dev = gates.reshape(GROUPS, TOK_DEV * TOP_K)
    cold_row, hot_row = jax.vmap(route_rows)(routes.reshape(GROUPS, TOK_DEV, TOP_K))
    cold_x, cold_do = jax.vmap(functools.partial(gather_rows, n_rows=N_EXPERTS * CAP_COLD))(cold_row, x_dev, dy_dev, gate_dev)
    hot_x, hot_do = jax.vmap(functools.partial(gather_rows, n_rows=N_HOT * CAP_HOT))(hot_row, x_dev, dy_dev, gate_dev)
    hot_ids = jnp.array([0, N_EXPERTS // 2])
    cold_out, cold_dx, grad_one, grad_three, grad_two = lax.map(run_expert, (
        by_expert(cold_x, N_EXPERTS, CAP_COLD), by_expert(cold_do, N_EXPERTS, CAP_COLD), w_in1, w_in3, w_out))
    hot_out, hot_dx, hot_one, hot_three, hot_two = lax.map(run_expert, (
        by_expert(hot_x, N_HOT, CAP_HOT), by_expert(hot_do, N_HOT, CAP_HOT),
        w_in1[hot_ids], w_in3[hot_ids], w_out[hot_ids]))
    y_out = jax.vmap(combine)(cold_row, hot_row, by_device(cold_out, N_EXPERTS, CAP_COLD),
                              by_device(hot_out, N_HOT, CAP_HOT), gate_dev)
    grad_x = jax.vmap(combine)(cold_row, hot_row, by_device(cold_dx, N_EXPERTS, CAP_COLD),
                               by_device(hot_dx, N_HOT, CAP_HOT), jnp.ones_like(gate_dev))
    return (y_out.reshape(TOK_PART, D_MODEL), grad_x.reshape(TOK_PART, D_MODEL),
            grad_one.at[hot_ids].add(hot_one), grad_three.at[hot_ids].add(hot_three),
            grad_two.at[hot_ids].add(hot_two))
```

```python
import functools

import jax
import jax.numpy as jnp
from jax import lax
from jax.experimental import pallas as pl
from jax.experimental.pallas import tpu as pltpu
from jax.sharding import PartitionSpec as P

N_HOT = 2
BF = jnp.bfloat16
F32 = jnp.float32
VMEM_LIMIT = 60 * 1024 * 1024


def value_a10(tok_dev, top_k, n_exp):
    cap_hot = 3 * tok_dev // 8
    cap_cold = max(8, ((tok_dev * top_k - N_HOT * cap_hot) // (n_exp - N_HOT) + 7) // 8 * 8)
    return cap_cold, cap_hot


def dot(a, b, ca=1, cb=0):
    return lax.dot_general(a, b, (((ca,), (cb,)), ((), ())), preferred_element_type=F32)


def params(n_axes):
    return pltpu.CompilerParams(dimension_semantics=("arbitrary",) * n_axes, vmem_limit_bytes=VMEM_LIMIT)


def cost(flops, nbytes):
    return pl.CostEstimate(flops=int(flops), bytes_accessed=int(nbytes), transcendentals=0)


def gather_body(caps, gated, rank_ref, *refs):
    if gated:
        gate_ref, src_ref, hot_ref, cold_ref = refs
    else:
        src_ref, hot_ref, cold_ref = refs
    tok_n = src_ref.shape[1]
    picks, scales = [], []
    for i, cap in enumerate(caps):
        hit = lax.broadcasted_iota(jnp.int32, (cap, tok_n), 0) == rank_ref[0, i:i + 1, :]
        picks.append(jnp.where(hit, 1.0, 0.0))
        if gated:
            scales.append(jnp.sum(jnp.where(hit, gate_ref[0, i:i + 1, :], 0.0), axis=1, keepdims=True))
    pick = jnp.concatenate(picks, axis=0).astype(BF)
    width = 256
    for n in range(src_ref.shape[2] // width):
        cols = pl.ds(n * width, width)
        rows = dot(pick, src_ref[0, :, cols])
        start = 0
        for i, cap in enumerate(caps):
            part = rows[start:start + cap]
            if gated:
                part = part * scales[i]
            part = part.astype(BF)
            if i == 0:
                hot_ref[0, :, cols] = part
            else:
                cold_ref[i - 1, 0, :, cols] = part
            start += cap


def gather_rows(caps, rank, gate, src):
    n_src, tok_n, d = src.shape
    n_loc = len(caps)
    table = pl.BlockSpec((1, n_loc, tok_n), lambda s: (s, 0, 0))
    ins = [rank] + ([gate] if gate is not None else []) + [src]
    return pl.pallas_call(
        functools.partial(gather_body, caps, gate is not None),
        grid=(n_src,),
        in_specs=[table] * (len(ins) - 1) + [pl.BlockSpec((1, tok_n, d), lambda s: (s, 0, 0))],
        out_specs=[pl.BlockSpec((1, caps[0], d), lambda s: (s, 0, 0)),
                   pl.BlockSpec((n_loc - 1, 1, caps[1], d), lambda s: (0, s, 0, 0))],
        out_shape=[jax.ShapeDtypeStruct((n_src, caps[0], d), BF),
                   jax.ShapeDtypeStruct((n_loc - 1, n_src, caps[1], d), BF)],
        compiler_params=params(1),
        cost_estimate=cost(2 * n_src * sum(caps) * tok_n * d, 2 * n_src * d * (tok_n + sum(caps))),
        name="gather_do" if gate is not None else "gather_x",
    )(*ins)


def fwd_body(x_ref, w1_ref, w3_ref, a_ref, b_ref):
    x = x_ref[0]
    a_ref[0] = dot(x, w1_ref[0]).astype(BF)
    b_ref[0] = dot(x, w3_ref[0]).astype(BF)


def expert_in(x_rows, w1, w3, m, off):
    n_e, n_r, d = x_rows.shape
    f = w1.shape[2]
    row = lambda width: pl.BlockSpec((1, m, width), lambda e, c: (e, c, 0))
    wsp = pl.BlockSpec((1, d, f), lambda e, c: (e + off, 0, 0))
    return pl.pallas_call(
        fwd_body, grid=(n_e, n_r // m), in_specs=[row(d), wsp, wsp], out_specs=[row(f), row(f)],
        out_shape=[jax.ShapeDtypeStruct((n_e, n_r, f), BF)] * 2, compiler_params=params(2),
        cost_estimate=cost(4 * n_e * n_r * d * f, 2 * n_e * n_r * (d + 2 * f)), name="expert_in",
    )(x_rows, w1, w3)


def hidden_of(a_ref, b_ref):
    a = a_ref[0].astype(F32)
    return (a * jax.nn.sigmoid(a) * b_ref[0].astype(F32)).astype(BF)


def out_body(q_ref, a_ref, b_ref, w2_ref, o_ref):
    o_ref[0] = dot(hidden_of(a_ref, b_ref), w2_ref[0]).astype(BF)


def own_out(q, a, b, w2, m, n_own, off):
    n_e, _, f = a.shape
    d = w2.shape[2]
    row = pl.BlockSpec((1, m, f), lambda e, c, q_ref: (e, q_ref[0] * n_own + c, 0))
    return pl.pallas_call(
        out_body,
        grid_spec=pltpu.PrefetchScalarGridSpec(
            num_scalar_prefetch=1, grid=(n_e, n_own),
            in_specs=[row, row, pl.BlockSpec((1, f, d), lambda e, c, q_ref: (e + off, 0, 0))],
            out_specs=pl.BlockSpec((1, m, d), lambda e, c, q_ref: (e, c, 0))),
        out_shape=jax.ShapeDtypeStruct((n_e, n_own * m, d), BF), compiler_params=params(2),
        cost_estimate=cost(2 * n_e * n_own * m * d * f, 2 * n_e * n_own * m * (d + 2 * f)), name="own_out",
    )(q, a, b, w2)


def back_of(do, a_ref, b_ref, w2):
    dh = dot(do, w2, 1, 1)
    a = a_ref[0].astype(F32)
    b = b_ref[0].astype(F32)
    sig = jax.nn.sigmoid(a)
    act = a * sig
    h = (act * b).astype(BF)
    db = (dh * a * sig).astype(BF)
    da = (dh * b * sig * (1.0 + a * (1.0 - sig))).astype(BF)
    return h, da, db


def own_back_body(q_ref, do_ref, a_ref, b_ref, w1_ref, w3_ref, w2_ref, dx_ref):
    _, da, db = back_of(do_ref[0], a_ref, b_ref, w2_ref[0])
    dx_ref[0] = (dot(da, w1_ref[0], 1, 1) + dot(db, w3_ref[0], 1, 1)).astype(BF)


def own_back(q, do, a, b, w1, w3, w2, m, n_own, off):
    n_e, _, f = a.shape
    d = w2.shape[2]
    row = lambda width: pl.BlockSpec((1, m, width), lambda e, c, q_ref: (e, q_ref[0] * n_own + c, 0))
    wsp = lambda s: pl.BlockSpec((1,) + s.shape[1:], lambda e, c, q_ref: (e + off, 0, 0))
    return pl.pallas_call(
        own_back_body,
        grid_spec=pltpu.PrefetchScalarGridSpec(
            num_scalar_prefetch=1, grid=(n_e, n_own),
            in_specs=[row(d), row(f), row(f), wsp(w1), wsp(w3), wsp(w2)],
            out_specs=pl.BlockSpec((1, m, d), lambda e, c, q_ref: (e, c, 0))),
        out_shape=jax.ShapeDtypeStruct((n_e, n_own * m, d), BF), compiler_params=params(2),
        cost_estimate=cost(6 * n_e * n_own * m * d * f, 2 * n_e * n_own * m * (2 * d + 2 * f)), name="own_back",
    )(q, do, a, b, w1, w3, w2)


def combine_body(caps, gated, slot_ref, *refs):
    if gated:
        gate_ref, hot_ref, cold_ref, y_ref = refs
    else:
        hot_ref, cold_ref, y_ref = refs
    n_rows = sum(caps)
    tok_n = y_ref.shape[0]
    col = lax.broadcasted_iota(jnp.int32, (tok_n, n_rows), 1)
    weight = jnp.zeros((tok_n, n_rows), F32)
    for i in range(len(caps)):
        gate = gate_ref[0, :, i:i + 1] if gated else 1.0
        weight = jnp.where(col == slot_ref[0, :, i:i + 1], gate, weight)
    terms = [weight.astype(BF)]
    if gated:
        rest = weight - terms[0].astype(F32)
        terms.append(rest.astype(BF))
        terms.append((rest - terms[1].astype(F32)).astype(BF))
    width = 256
    for n in range(y_ref.shape[1] // width):
        cols = pl.ds(n * width, width)
        rows = jnp.concatenate(
            [hot_ref[0, :, cols].astype(F32)] + [cold_ref[i, 0, :, cols].astype(F32) for i in range(len(caps) - 1)],
            axis=0).astype(BF)
        total = dot(terms[0], rows)
        for term in terms[1:]:
            total = total + dot(term, rows)
        y_ref[:, cols] = total


def combine(caps, slot, gate, hot, cold):
    n_src, cap_hot, d = hot.shape
    tok_n = slot.shape[1]
    n_loc = len(caps)
    table = pl.BlockSpec((1, tok_n, n_loc), lambda s: (s, 0, 0))
    tables = [slot] + ([gate] if gate is not None else [])
    return pl.pallas_call(
        functools.partial(combine_body, caps, gate is not None),
        grid=(n_src,),
        in_specs=[table] * len(tables) + [
            pl.BlockSpec((1, cap_hot, d), lambda s: (s, 0, 0)),
            pl.BlockSpec((n_loc - 1, 1, caps[1], d), lambda s: (0, s, 0, 0))],
        out_specs=pl.BlockSpec((tok_n, d), lambda s: (s, 0)),
        out_shape=jax.ShapeDtypeStruct((n_src * tok_n, d), F32), compiler_params=params(1),
        cost_estimate=cost((6 if gate is not None else 2) * n_src * tok_n * sum(caps) * d,
                           n_src * d * (4 * tok_n + 2 * sum(caps))),
        name="combine_y" if gate is not None else "combine_dx",
    )(*tables, hot, cold)


def hot_grad_body(x_ref, do_ref, a_ref, b_ref, w2_ref, g1_ref, g3_ref, g2_ref):
    h, da, db = back_of(do_ref[0], a_ref, b_ref, w2_ref[0])
    x = x_ref[0]
    parts = dot(x, da, 0, 0), dot(x, db, 0, 0), dot(h, do_ref[0], 0, 0)

    @pl.when(pl.program_id(0) == 0)
    def _():
        for ref, part in zip((g1_ref, g3_ref, g2_ref), parts):
            ref[0] = part

    @pl.when(pl.program_id(0) > 0)
    def _():
        for ref, part in zip((g1_ref, g3_ref, g2_ref), parts):
            ref[0] += part


def hot_grads(x, do, a, b, w1, w2, m):
    n_r, d = x.shape[1:]
    f = a.shape[2]
    row = lambda width: pl.BlockSpec((1, m, width), lambda c: (0, c, 0))
    first = lambda s: pl.BlockSpec((1,) + s.shape[1:], lambda c: (0, 0, 0))
    shapes = [jax.ShapeDtypeStruct(w1.shape, F32), jax.ShapeDtypeStruct(w1.shape, F32),
              jax.ShapeDtypeStruct(w2.shape, F32)]
    return pl.pallas_call(
        hot_grad_body, grid=(n_r // m,), in_specs=[row(d), row(d), row(f), row(f), first(w2)],
        out_specs=[first(s) for s in shapes], out_shape=shapes, compiler_params=params(1),
        cost_estimate=cost(8 * n_r * d * f, 2 * n_r * (2 * d + 2 * f)), name="hot_grads",
    )(x, do, a, b, w2)


def cold_grad_body(n_chunk, *refs):
    (chunk_ref, a_ref, b_ref, w2_ref, x_ref, do_ref, _, _, _, g1_ref, g3_ref, g2_ref, h_s, da_s, db_s) = refs
    step = pl.program_id(1)
    m = chunk_ref.shape[1]

    @pl.when(step < n_chunk)
    def _():
        h, da, db = back_of(chunk_ref[0], a_ref, b_ref, w2_ref[0])
        rows = pl.ds(pl.multiple_of(step * m, m), m)
        h_s[rows, :] = h
        da_s[rows, :] = da
        db_s[rows, :] = db

    @pl.when(step >= n_chunk)
    def _():
        x = x_ref[0]
        g1_ref[0] = dot(x, da_s[...], 0, 0)
        g3_ref[0] = dot(x, db_s[...], 0, 0)
        g2_ref[0] = dot(h_s[...], do_ref[0], 0, 0)


def cold_grads(grads, x, do, a, b, w2, m, tile, off):
    n_e, n_r, d = x.shape
    f = a.shape[2]
    n_chunk, n_tile = n_r // m, d // tile
    chunk = lambda width: pl.BlockSpec((1, m, width), lambda e, s: (e, jnp.minimum(s, n_chunk - 1), 0))
    place = lambda s: jnp.maximum(s - n_chunk, 0)
    tiles = pl.BlockSpec((1, n_r, tile), lambda e, s: (e, 0, place(s)))
    any_spec = pl.BlockSpec(memory_space=pl.ANY)
    rows_out = pl.BlockSpec((1, tile, f), lambda e, s: (e + off, place(s), 0))
    cols_out = pl.BlockSpec((1, f, tile), lambda e, s: (e + off, 0, place(s)))
    return pl.pallas_call(
        functools.partial(cold_grad_body, n_chunk),
        grid=(n_e, n_chunk + n_tile),
        in_specs=[chunk(d), chunk(f), chunk(f), pl.BlockSpec((1, f, d), lambda e, s: (e + off, 0, 0)),
                  tiles, tiles, any_spec, any_spec, any_spec],
        out_specs=[rows_out, rows_out, cols_out],
        out_shape=[jax.ShapeDtypeStruct(g.shape, F32) for g in grads],
        scratch_shapes=[pltpu.VMEM((n_r, f), BF)] * 3,
        input_output_aliases={6: 0, 7: 1, 8: 2}, compiler_params=params(2),
        cost_estimate=cost(8 * n_e * n_r * d * f, 2 * n_e * n_r * (3 * d + 2 * f)), name="cold_grads",
    )(do, a, b, w2, x, do, *grads)


def solution(mesh):
    n_dev = mesh.shape['expert']
    n_data = mesh.shape['data']
    row_spec = P(('pod', 'data', 'expert'), None)
    w_spec = P('expert', None, None)
    grad_spec = P(('pod', 'expert'), None, None)
    both = ('data', 'expert')

    def body(tokens, routes, gates, grad_y, w_in1, w_in3, w_out):
        tok_n, d_model = tokens.shape
        top_k = routes.shape[1]
        n_loc = w_in1.shape[0]
        n_exp = n_loc * n_dev
        n_src = n_data * n_dev
        cap_cold, cap_hot = value_a10(tok_n, top_k, n_exp)
        assert (n_exp // 2) % n_loc == 0
        caps = (cap_hot,) + (cap_cold,) * (n_loc - 1)
        offs = [0] + [cap_hot + i * cap_cold for i in range(n_loc - 1)]
        q = lax.axis_index('data')
        q_arr = jnp.reshape(q, (1,)).astype(jnp.int32)

        local = jnp.concatenate([routes.T.astype(F32), gates.T], axis=0)
        tables = lax.all_gather(local, both, axis=0, tiled=True).reshape(n_src, 2 * top_k, tok_n)
        x_all = lax.all_gather(tokens, both, axis=0, tiled=True).reshape(n_src, tok_n, d_model)
        dy_all = lax.all_gather(grad_y, both, axis=0, tiled=True).reshape(n_src, tok_n, d_model)
        ids = lax.axis_index('expert') * n_loc + jnp.arange(n_loc)
        match = tables[:, :top_k, None, :] == ids.astype(F32)[None, None, :, None]
        hit = jnp.any(match, axis=1)
        gate = jnp.sum(jnp.where(match, tables[:, top_k:, None, :], 0.0), axis=1)
        before = (jnp.arange(tok_n)[:, None] < jnp.arange(tok_n)[None, :]).astype(BF)
        rank = jnp.einsum('sit,tu->siu', hit.astype(BF), before, preferred_element_type=F32).astype(jnp.int32)
        cap_here = jnp.where((ids == 0) | (ids == n_exp // 2), cap_hot, cap_cold)
        rank = jnp.where(hit & (rank < cap_here[None, :, None]), rank, -1)
        own = lambda t: lax.dynamic_slice_in_dim(t, q * n_dev, n_dev, 0).transpose(0, 2, 1)
        rank_own = own(rank)
        slot_own = jnp.where(rank_own >= 0, rank_own + jnp.array(offs, jnp.int32), -1)
        gate_own = own(gate)

        m_cold, m_hot = n_dev * cap_cold, n_dev * cap_hot // 2
        xh, xc = gather_rows(caps, rank, None, x_all)
        xh = xh.reshape(1, n_src * cap_hot, d_model)
        xc = xc.reshape(n_loc - 1, n_src * cap_cold, d_model)
        ac, bc = expert_in(xc, w_in1, w_in3, m_cold, 1)
        ah, bh = expert_in(xh, w_in1, w_in3, m_hot, 0)
        oc = own_out(q_arr, ac, bc, w_out, m_cold, 1, 1).reshape(n_loc - 1, n_dev, cap_cold, d_model)
        oh = own_out(q_arr, ah, bh, w_out, m_hot, 2, 0).reshape(n_dev, cap_hot, d_model)
        y_part = combine(caps, slot_own, gate_own, oh, oc)
        y_out = lax.psum_scatter(y_part, 'expert', scatter_dimension=0, tiled=True).astype(BF)

        doh, doc = gather_rows(caps, rank, gate, dy_all)
        doh = doh.reshape(1, n_src * cap_hot, d_model)
        doc = doc.reshape(n_loc - 1, n_src * cap_cold, d_model)
        dxc = own_back(q_arr, doc, ac, bc, w_in1, w_in3, w_out, m_cold, 1, 1)
        dxh = own_back(q_arr, doh, ah, bh, w_in1, w_in3, w_out, m_hot, 2, 0)
        dx_part = combine(caps, slot_own, None, dxh.reshape(n_dev, cap_hot, d_model),
                          dxc.reshape(n_loc - 1, n_dev, cap_cold, d_model))
        grad_x = lax.psum_scatter(dx_part, 'expert', scatter_dimension=0, tiled=True).astype(BF)

        grads = hot_grads(xh, doh, ah, bh, w_in1, w_out, m_hot)
        grads = cold_grads(grads, xc, doc, ac, bc, w_out, m_cold, d_model // 3, 1)
        return (y_out, grad_x) + tuple(grads)

    return jax.shard_map(body, mesh=mesh,
                         in_specs=(row_spec, row_spec, row_spec, row_spec, w_spec, w_spec, w_spec),
                         out_specs=(row_spec, row_spec, grad_spec, grad_spec, grad_spec),
                         check_vma=False)
```

```python
import functools

import jax
import jax.numpy as jnp
from jax import lax
from jax.experimental import pallas as pl
from jax.experimental.pallas import tpu as pltpu
from jax.sharding import PartitionSpec as P

N_HOT = 2
BF = jnp.bfloat16
F32 = jnp.float32
VMEM_LIMIT = 60 * 1024 * 1024


def value_a10(tok_dev, top_k, n_exp):
    cap_hot = 3 * tok_dev // 8
    cap_cold = max(8, ((tok_dev * top_k - N_HOT * cap_hot) // (n_exp - N_HOT) + 7) // 8 * 8)
    return cap_cold, cap_hot


def dot(a, b, ca=1, cb=0):
    return lax.dot_general(a, b, (((ca,), (cb,)), ((), ())), preferred_element_type=F32)


def params(n_axes):
    return pltpu.CompilerParams(dimension_semantics=("arbitrary",) * n_axes, vmem_limit_bytes=VMEM_LIMIT)


def cost(flops, nbytes):
    return pl.CostEstimate(flops=int(flops), bytes_accessed=int(nbytes), transcendentals=0)


def gather_body(caps, gated, n_half, rank_ref, *refs):
    if gated:
        gate_ref, src_ref, rows_ref, buf, sem = refs
    else:
        src_ref, rows_ref, buf, sem = refs
    step = pl.program_id(0)
    n_src_step, tok_n, d = src_ref.shape
    blk = caps[-1]
    slot = lax.rem(step, 2)

    def copies(step_i, slot_i):
        out = []
        for k in range(n_src_step):
            s = step_i * n_src_step + k
            half = s // n_half
            out.append(pltpu.make_async_copy(
                buf.at[slot_i, k, pl.ds(0, 2)], rows_ref.at[half, pl.ds(2 * (s - half * n_half), 2)], sem.at[slot_i]))
            out.append(pltpu.make_async_copy(
                buf.at[slot_i, k, pl.ds(2, len(caps) - 1)], rows_ref.at[pl.ds(2, len(caps) - 1), s], sem.at[slot_i]))
        return out

    @pl.when(step >= 2)
    def _():
        for c in copies(step - 2, slot):
            c.wait()

    for k in range(n_src_step):
        picks, scales = [], []
        for i, cap in enumerate(caps):
            hit = lax.broadcasted_iota(jnp.int32, (cap, tok_n), 0) == rank_ref[k, i:i + 1, :]
            picks.append(jnp.where(hit, 1.0, 0.0))
            if gated:
                scales.append(jnp.sum(jnp.where(hit, gate_ref[k, i:i + 1, :], 0.0), axis=1, keepdims=True))
        pick = jnp.concatenate(picks, axis=0).astype(BF)
        scale = jnp.concatenate(scales, axis=0) if gated else None
        width = 256
        for n in range(d // width):
            cols = pl.ds(n * width, width)
            rows = dot(pick, src_ref[k, :, cols])
            if gated:
                rows = rows * scale
            for j in range(sum(caps) // blk):
                buf[slot, k, j, :, cols] = rows[j * blk:(j + 1) * blk].astype(BF)

    for c in copies(step, slot):
        c.start()

    @pl.when(step == pl.num_programs(0) - 1)
    def _():
        for c in copies(step - 1, 1 - slot):
            c.wait()
        for c in copies(step, slot):
            c.wait()


def gather_rows(caps, rank, gate, src):
    n_src, tok_n, d = src.shape
    n_loc = len(caps)
    blk = caps[-1]
    per = 2
    assert caps[0] == 2 * blk and n_src % (2 * per) == 0 and n_src // per >= 2
    table = pl.BlockSpec((per, n_loc, tok_n), lambda s: (s, 0, 0))
    ins = [rank] + ([gate] if gate is not None else []) + [src]
    return pl.pallas_call(
        functools.partial(gather_body, caps, gate is not None, n_src // 2),
        grid=(n_src // per,),
        in_specs=[table] * (len(ins) - 1) + [pl.BlockSpec((per, tok_n, d), lambda s: (s, 0, 0))],
        out_specs=pl.BlockSpec(memory_space=pl.ANY),
        out_shape=jax.ShapeDtypeStruct((n_loc + 1, n_src, blk, d), BF),
        scratch_shapes=[pltpu.VMEM((2, per, n_loc + 1, blk, d), BF), pltpu.SemaphoreType.DMA((2,))],
        compiler_params=params(1),
        cost_estimate=cost(2 * n_src * sum(caps) * tok_n * d, 2 * n_src * d * (tok_n + sum(caps))),
        name="gather_do" if gate is not None else "gather_x",
    )(*ins).reshape(n_loc + 1, n_src * blk, d)


def own_chunk(i, q, n_chunk):
    hot = i < 2
    return jnp.where(hot, 2 * q // n_chunk, i), jnp.where(hot, 2 * q % n_chunk + i, q)


def expert_of(e):
    return jnp.maximum(e - 1, 0)


def fwd_body(n_chunk, q_ref, x_ref, w1_ref, w3_ref, w2_ref, a_ref, b_ref, o_ref):
    e, c, q = pl.program_id(0), pl.program_id(1), q_ref[0]
    x = x_ref[0]
    a_ref[0] = dot(x, w1_ref[0]).astype(BF)
    b_ref[0] = dot(x, w3_ref[0]).astype(BF)
    own = jnp.where(e < 2, e * n_chunk + c - 2 * q, jnp.where(c == q, 0, 2))

    @pl.when((own == 0) | (own == 1))
    def _():
        a = a_ref[0].astype(F32)
        h = (a * jax.nn.sigmoid(a) * b_ref[0].astype(F32)).astype(BF)
        o_ref[0] = dot(h, w2_ref[0]).astype(BF)


def expert_in(q, x_rows, w1, w3, w2, m):
    n_e, n_r, d = x_rows.shape
    f = w1.shape[2]
    row = lambda width: pl.BlockSpec((1, m, width), lambda e, c, q_ref: (e, c, 0))
    wsp = lambda s: pl.BlockSpec((1,) + s.shape[1:], lambda e, c, q_ref: (expert_of(e), 0, 0))

    n_chunk = n_r // m

    def out_slot(e, c, q_ref):
        return (jnp.where(e < 2, jnp.clip(e * n_chunk + c - 2 * q_ref[0], 0, 1), e), 0, 0)

    return pl.pallas_call(
        functools.partial(fwd_body, n_chunk),
        grid_spec=pltpu.PrefetchScalarGridSpec(
            num_scalar_prefetch=1, grid=(n_e, n_chunk), in_specs=[row(d), wsp(w1), wsp(w3), wsp(w2)],
            out_specs=[row(f), row(f), pl.BlockSpec((1, m, d), out_slot)]),
        out_shape=[jax.ShapeDtypeStruct((n_e, n_r, f), BF)] * 2 + [jax.ShapeDtypeStruct((n_e, m, d), BF)],
        compiler_params=params(2),
        cost_estimate=cost(4 * n_e * n_r * d * f, 2 * n_e * n_r * (d + 2 * f)), name="expert_in",
    )(q, x_rows, w1, w3, w2)


def back_of(do, a_ref, b_ref, w2):
    dh = dot(do, w2, 1, 1)
    a = a_ref[0].astype(F32)
    b = b_ref[0].astype(F32)
    sig = jax.nn.sigmoid(a)
    act = a * sig
    h = (act * b).astype(BF)
    db = (dh * a * sig).astype(BF)
    da = (dh * b * sig * (1.0 + a * (1.0 - sig))).astype(BF)
    return h, da, db


def own_back_body(q_ref, do_ref, a_ref, b_ref, w1_ref, w3_ref, w2_ref, dx_ref):
    _, da, db = back_of(do_ref[0], a_ref, b_ref, w2_ref[0])
    dx_ref[0] = (dot(da, w1_ref[0], 1, 1) + dot(db, w3_ref[0], 1, 1)).astype(BF)


def own_back(q, do, a, b, w1, w3, w2, m):
    n_e, _, f = a.shape
    d = w2.shape[2]
    n_chunk = a.shape[1] // m
    row = lambda width: pl.BlockSpec((1, m, width), lambda i, q_ref: own_chunk(i, q_ref[0], n_chunk) + (0,))
    wsp = lambda s: pl.BlockSpec((1,) + s.shape[1:], lambda i, q_ref: (expert_of(i), 0, 0))
    return pl.pallas_call(
        own_back_body,
        grid_spec=pltpu.PrefetchScalarGridSpec(
            num_scalar_prefetch=1, grid=(n_e,),
            in_specs=[row(d), row(f), row(f), wsp(w1), wsp(w3), wsp(w2)],
            out_specs=pl.BlockSpec((1, m, d), lambda i, q_ref: (i, 0, 0))),
        out_shape=jax.ShapeDtypeStruct((n_e, m, d), BF), compiler_params=params(1),
        cost_estimate=cost(6 * n_e * m * d * f, 2 * n_e * m * (2 * d + 2 * f)), name="own_back",
    )(q, do, a, b, w1, w3, w2)


def combine_body(caps, gated, slot_ref, *refs):
    n_loc = len(caps)
    gate_ref = refs[0] if gated else None
    row_refs, y_ref = refs[gated:gated + n_loc], refs[gated + n_loc]
    n_rows = sum(caps)
    tok_n = y_ref.shape[0]
    col = lax.broadcasted_iota(jnp.int32, (tok_n, n_rows), 1)
    weight = jnp.zeros((tok_n, n_rows), F32)
    for i in range(n_loc):
        gate = gate_ref[0, :, i:i + 1] if gated else 1.0
        weight = jnp.where(col == slot_ref[0, :, i:i + 1], gate, weight)
    terms = [weight.astype(BF)]
    if gated:
        rest = weight - terms[0].astype(F32)
        terms.append(rest.astype(BF))
        terms.append((rest - terms[1].astype(F32)).astype(BF))
    width = 256
    for n in range(y_ref.shape[1] // width):
        cols = pl.ds(n * width, width)
        rows = jnp.concatenate(
            [ref[0, j, :, cols].astype(F32) for ref in row_refs for j in range(ref.shape[1])], axis=0).astype(BF)
        total = dot(terms[0], rows)
        for term in terms[1:]:
            total = total + dot(term, rows)
        y_ref[:, cols] = total


def combine(caps, slot, gate, rows):
    n_src, tok_n, n_loc = slot.shape
    d = rows.shape[2]
    blk = caps[-1]
    rows = rows.reshape(n_loc + 1, n_src, blk, d)
    table = pl.BlockSpec((1, tok_n, n_loc), lambda s: (s, 0, 0))
    tables = [slot] + ([gate] if gate is not None else [])
    hot = pl.BlockSpec((1, 2, blk, d), lambda s: (s // (n_src // 2), s % (n_src // 2), 0, 0))
    colds = [pl.BlockSpec((1, 1, blk, d), lambda s, i=i: (2 + i, s, 0, 0)) for i in range(n_loc - 1)]
    return pl.pallas_call(
        functools.partial(combine_body, caps, gate is not None),
        grid=(n_src,),
        in_specs=[table] * len(tables) + [hot] + colds,
        out_specs=pl.BlockSpec((tok_n, d), lambda s: (s, 0)),
        out_shape=jax.ShapeDtypeStruct((n_src * tok_n, d), F32), compiler_params=params(1),
        cost_estimate=cost((6 if gate is not None else 2) * n_src * tok_n * sum(caps) * d,
                           n_src * d * (4 * tok_n + 2 * sum(caps))),
        name="combine_y" if gate is not None else "combine_dx",
    )(*tables, *([rows] * n_loc))


def grad_body(n_chunk, chunk_ref, a_ref, b_ref, w2_ref, x_ref, do_ref, g1_ref, g3_ref, g2_ref,
              h_s, da_s, db_s, acc):
    e, step = pl.program_id(0), pl.program_id(1)
    m = chunk_ref.shape[1]
    outs = (g1_ref, g3_ref, g2_ref)

    @pl.when(step < n_chunk)
    def _():
        h, da, db = back_of(chunk_ref[0], a_ref, b_ref, w2_ref[0])
        rows = pl.ds(pl.multiple_of(step * m, m), m)
        h_s[rows, :] = h
        da_s[rows, :] = da
        db_s[rows, :] = db

    @pl.when(step >= n_chunk)
    def _():
        x = x_ref[0]
        g1_ref[0] = dot(x, da_s[...], 0, 0)
        g3_ref[0] = dot(x, db_s[...], 0, 0)
        g2_ref[0] = dot(h_s[...], do_ref[0], 0, 0)
        tile = step - n_chunk

        @pl.when(e == 0)
        def _():
            for k, ref in enumerate(outs):
                acc[k, tile] = ref[0]

        @pl.when(e == 1)
        def _():
            for k, ref in enumerate(outs):
                ref[0] += acc[k, tile]


def expert_grads(x, do, a, b, w1, w2, m, tile):
    n_e, n_r, d = x.shape
    f = a.shape[2]
    assert tile == f
    n_chunk, n_tile = n_r // m, d // tile
    chunk = lambda width: pl.BlockSpec((1, m, width), lambda e, s: (e, jnp.minimum(s, n_chunk - 1), 0))
    place = lambda s: jnp.maximum(s - n_chunk, 0)
    tiles = pl.BlockSpec((1, n_r, tile), lambda e, s: (e, 0, place(s)))
    out_place = lambda e, s: jnp.where(e == 0, 0, place(s))
    rows_out = pl.BlockSpec((1, tile, f), lambda e, s: (expert_of(e), out_place(e, s), 0))
    cols_out = pl.BlockSpec((1, f, tile), lambda e, s: (expert_of(e), 0, out_place(e, s)))
    return pl.pallas_call(
        functools.partial(grad_body, n_chunk),
        grid=(n_e, n_chunk + n_tile),
        in_specs=[chunk(d), chunk(f), chunk(f), pl.BlockSpec((1, f, d), lambda e, s: (expert_of(e), 0, 0)),
                  tiles, tiles],
        out_specs=[rows_out, rows_out, cols_out],
        out_shape=[jax.ShapeDtypeStruct(w.shape, F32) for w in (w1, w1, w2)],
        scratch_shapes=[pltpu.VMEM((n_r, f), BF)] * 3 + [pltpu.VMEM((3, n_tile, tile, f), F32)],
        compiler_params=params(2),
        cost_estimate=cost(8 * n_e * n_r * d * f, 2 * n_e * n_r * (3 * d + 2 * f)), name="expert_grads",
    )(do, a, b, w2, x, do)


def solution(mesh):
    n_dev = mesh.shape['expert']
    n_data = mesh.shape['data']
    row_spec = P(('pod', 'data', 'expert'), None)
    w_spec = P('expert', None, None)
    grad_spec = P(('pod', 'expert'), None, None)
    both = ('data', 'expert')

    def body(tokens, routes, gates, grad_y, w_in1, w_in3, w_out):
        tok_n, d_model = tokens.shape
        top_k = routes.shape[1]
        n_loc = w_in1.shape[0]
        n_exp = n_loc * n_dev
        n_src = n_data * n_dev
        cap_cold, cap_hot = value_a10(tok_n, top_k, n_exp)
        assert (n_exp // 2) % n_loc == 0
        caps = (2 * cap_cold,) + (cap_cold,) * (n_loc - 1)
        assert cap_hot <= caps[0]
        offs = [0] + [(i + 2) * cap_cold for i in range(n_loc - 1)]
        q = lax.axis_index('data')
        q_arr = jnp.reshape(q, (1,)).astype(jnp.int32)

        routes_all = lax.all_gather(routes.T, both, axis=0, tiled=True).reshape(n_src, top_k, tok_n)
        gates_all = lax.all_gather(gates.T, both, axis=0, tiled=True).reshape(n_src, top_k, tok_n)
        x_all = lax.all_gather(tokens, both, axis=0, tiled=True).reshape(n_src, tok_n, d_model)
        dy_all = lax.all_gather(grad_y, both, axis=0, tiled=True).reshape(n_src, tok_n, d_model)
        ids = lax.axis_index('expert') * n_loc + jnp.arange(n_loc)
        match = routes_all[:, :, None, :] == ids[None, None, :, None]
        hit = jnp.any(match, axis=1)
        gate = jnp.sum(jnp.where(match, gates_all[:, :, None, :], 0.0), axis=1)
        before = (jnp.arange(tok_n)[:, None] < jnp.arange(tok_n)[None, :]).astype(BF)
        rank = jnp.einsum('sit,tu->siu', hit.astype(BF), before, preferred_element_type=F32).astype(jnp.int32)
        cap_here = jnp.where((ids == 0) | (ids == n_exp // 2), cap_hot, cap_cold)
        rank = jnp.where(hit & (rank < cap_here[None, :, None]), rank, -1)
        own = lambda t: lax.dynamic_slice_in_dim(t, q * n_dev, n_dev, 0).transpose(0, 2, 1)
        rank_own = own(rank)
        slot_own = jnp.where(rank_own >= 0, rank_own + jnp.array(offs, jnp.int32), -1)
        gate_own = own(gate)

        m = n_dev * cap_cold
        x_rows = gather_rows(caps, rank, None, x_all)
        a, b, o = expert_in(q_arr, x_rows, w_in1, w_in3, w_out, m)
        y_part = combine(caps, slot_own, gate_own, o)
        y_out = lax.psum_scatter(y_part, 'expert', scatter_dimension=0, tiled=True).astype(BF)

        do_rows = gather_rows(caps, rank, gate, dy_all)
        dx = own_back(q_arr, do_rows, a, b, w_in1, w_in3, w_out, m)
        dx_part = combine(caps, slot_own, None, dx)
        grad_x = lax.psum_scatter(dx_part, 'expert', scatter_dimension=0, tiled=True).astype(BF)

        grads = expert_grads(x_rows, do_rows, a, b, w_in1, w_out, m, w_in1.shape[2])
        return (y_out, grad_x) + tuple(grads)

    return jax.shard_map(body, mesh=mesh,
                         in_specs=(row_spec, row_spec, row_spec, row_spec, w_spec, w_spec, w_spec),
                         out_specs=(row_spec, row_spec, grad_spec, grad_spec, grad_spec),
                         check_vma=False)
```
